256 devices in a mesh: dp: 4 (over z_hi, core), head: 64 (over x, y, z_lo).
Axes of the slice: x: 4, y: 4, z: 8 (z_hi: 2, z_lo: 4; z = z_hi * 4 + z_lo), core: 2. Of those that a mesh axis runs over, the one named last changes fastest.
Arguments:
- query_nope: bfloat16 [2, 4096, 2048], P(None, ('dp', 'head')), may hold values from -12 to 12
- query_rope: bfloat16 [2, 4096, 1024], P(None, ('dp', 'head')), may hold values from -640 to 640
- key_up: bfloat16 [2, 16, 128, 512], P(None, 'dp'), may hold values from -0.5 to 0.5
- value_up: bfloat16 [2, 16, 512, 128], P(None, 'dp'), may hold values from -0.25 to 0.25
- pool_latent: bfloat16 [2, 64, 128, 512], P(None, 'head'), may hold values from -6 to 6
- pool_rope: bfloat16 [2, 64, 64, 128], P(None, 'head'), may hold values from -8 to 8
- block_table: int32 [2, 48], replicated, may hold values from 0 to 63, as said below
- suffix_latent: bfloat16 [2, 4096, 128, 512], P(None, ('dp', 'head')), may hold values from -8 to 8
- suffix_rope: bfloat16 [2, 4096, 64, 128], P(None, ('dp', 'head')), may hold values from -8 to 8
- lengths: int32 [4096], P(('dp', 'head')), may hold values from 1 to 128, as said below
Outputs:
- attention: bfloat16 [2, 4096, 2048], P(None, ('dp', 'head'))
The draws below stay inside these ranges and needn't reach their ends.
Inputs may be any that keep to these rules, and one draw needn't show every extreme that they name: `block_table`: each row names 48 different slots. `lengths`: among the 16 sequences of every device at least one has length 128.
All inputs are finite; a program needn't handle non-finite values.
Results may differ from the reference program's by a relative error of at most 0.0087.
Values may be sent and summed in bfloat16 or wider, within the bound.
No kernel may reach another device: no remote copies, remote signals or barrier semaphores. Data moves between devices by JAX's collectives and lax.ppermute only.
A program may use at most 128 MiB of HBM per device.

```python
import jax
import jax.numpy as jnp
from jax import lax

HEADS = 16
RANK = 512
NOPE = 128
ROPE = 64
VDIM = 128
LAYERS = 2
SEQ_DEV = 16
SUF = 128
BLK = 128
POOL = 64
NBLK = 48
PREFIX = 6144
SEQS = 4096


def slot_table(key):
    layer_keys = jax.random.split(jax.random.fold_in(key, 7), LAYERS)
    chosen = jax.vmap(lambda item_key: jax.random.permutation(item_key, POOL)[:NBLK])(layer_keys)
    return chosen.astype(jnp.int32)


def rope_base(key):
    noise = jax.random.normal(jax.random.fold_in(key, 21), (LAYERS, POOL, ROPE, BLK), jnp.float32)
    return jnp.clip(noise, -4.0, 4.0)


def unit_keys(key):
    base = rope_base(key)
    return base


def draw_block_table(key, part):
    return slot_table(key)


def draw_lengths(key, part):
    first_key, second_key = jax.random.split(jax.random.fold_in(key, 41))
    drawn = jax.random.randint(first_key, (SEQS,), 1, SUF + 1)
    devices_count = SEQS // SEQ_DEV
    full_pick = jax.random.randint(second_key, (devices_count,), 0, SEQ_DEV)
    positions = jnp.arange(devices_count) * SEQ_DEV + full_pick
    return drawn.at[positions].set(SUF).astype(jnp.int32)


def draw_pool_rope(key, part):
    base = unit_keys(key)
    return base.astype(jnp.bfloat16)


def draw_query_rope(key, part):
    noise = jax.random.normal(jax.random.fold_in(key, 23), (LAYERS, SEQS, HEADS * ROPE), jnp.float32)
    values = jnp.clip(2.0 * noise, -12.0, 12.0)
    return values.astype(jnp.bfloat16)


def draw_query_nope(key, part):
    noise = jax.random.normal(jax.random.fold_in(key, 25), (LAYERS, SEQS, HEADS * NOPE), jnp.float32)
    values = jnp.clip(2.0 * noise, -12.0, 12.0)
    return values.astype(jnp.bfloat16)


def levels(key, shape, shards, smallest, top_value):
    factor_of = 1.0
    for axis_at, parts in shards:
        steps = jax.random.uniform(jax.random.fold_in(jax.random.fold_in(key, 6), axis_at), (parts,), jnp.float32, smallest / len(shards), top_value / len(shards))
        factor_of = factor_of * jnp.repeat(jnp.exp(steps), shape[axis_at] // parts).reshape((-1,) + (1,) * (len(shape) - 1 - axis_at))
    return factor_of


def centred(stream_key, dims, scale, reach, shards=(), kind=jnp.bfloat16):
    loudness = levels(stream_key, dims, shards, -0.22, 0.18) if shards else 1.0
    result = jax.random.normal(stream_key, dims, jnp.float32) * scale * loudness
    return jnp.minimum(jnp.maximum(result, -reach), reach).astype(kind)


def setup_inputs(seed: int = 0) -> dict:
    key_list = jax.random.split(jax.random.key(seed), 11)
    return {
        "query_nope": draw_query_nope(jax.random.fold_in(key_list[10], 71), 0),
        "query_rope": draw_query_rope(jax.random.fold_in(key_list[10], 71), 0),
        "key_up": centred(key_list[2], (LAYERS, HEADS, NOPE, RANK), NOPE ** -0.5, 0.5, ((1, 4),)),
        "value_up": centred(key_list[3], (LAYERS, HEADS, RANK, VDIM), RANK ** -0.5, 0.25, ((1, 4),)),
        "pool_latent": centred(key_list[4], (LAYERS, POOL, BLK, RANK), 1.0, 6.0, ((1, 64),)),
        "pool_rope": draw_pool_rope(jax.random.fold_in(key_list[10], 71), 0),
        "block_table": draw_block_table(jax.random.fold_in(key_list[10], 71), 0),
        "suffix_latent": centred(key_list[7], (LAYERS, SEQS, SUF, RANK), 1.25, 8.0, ((1, 256),)),
        "suffix_rope": centred(key_list[8], (LAYERS, SEQS, ROPE, SUF), 1.25, 8.0, ((1, 256),)),
        "lengths": draw_lengths(jax.random.fold_in(key_list[10], 71), 0),
    }


def rounded(values):
    return lax.optimization_barrier(values.astype(jnp.bfloat16)).astype(jnp.float32)


def reference(query_nope, query_rope, key_up, value_up, pool_latent, pool_rope, block_table, suffix_latent, suffix_rope, lengths):
    scale = (NOPE + ROPE) ** -0.5
    groups = SEQS // SEQ_DEV
    results = []
    for layer_index in range(LAYERS):
        chosen = block_table[layer_index].astype(jnp.int32)
        prefix_latent = pool_latent[layer_index][chosen].reshape(PREFIX, RANK).astype(jnp.float32)
        prefix_rope = jnp.transpose(pool_rope[layer_index][chosen], (1, 0, 2)).reshape(ROPE, PREFIX).astype(jnp.float32)
        key_weight = key_up[layer_index].astype(jnp.float32)
        value_weight = value_up[layer_index].astype(jnp.float32)

        def one_block(items):
            query_heads, query_rotary, own_latent, own_rope, seq_lengths = items
            query_heads = query_heads.astype(jnp.float32)
            query_rotary = query_rotary.astype(jnp.float32)
            own_latent = own_latent.astype(jnp.float32)
            own_rope = own_rope.astype(jnp.float32)
            q_latent = rounded(jnp.einsum('bhd,hdc->bhc', query_heads, key_weight))
            prefix_scores = (jnp.einsum('bhc,tc->bht', q_latent, prefix_latent) + jnp.einsum('bhr,rt->bht', query_rotary, prefix_rope)) * scale
            suffix_scores = (jnp.einsum('bhc,btc->bht', q_latent, own_latent) + jnp.einsum('bhr,brt->bht', query_rotary, own_rope)) * scale
            live_mask = (jnp.arange(SUF)[None, :] < seq_lengths[:, None])[:, None, :]
            row_max = jnp.maximum(jnp.max(prefix_scores, axis=-1), jnp.max(jnp.where(live_mask, suffix_scores, -jnp.inf), axis=-1))
            prefix_exp = jnp.exp(prefix_scores - row_max[..., None])
            suffix_exp = jnp.where(live_mask, jnp.exp(suffix_scores - row_max[..., None]), 0.0)
            row_total = jnp.sum(prefix_exp, axis=-1) + jnp.sum(suffix_exp, axis=-1)
            gathered = jnp.einsum('bht,tc->bhc', rounded(prefix_exp), prefix_latent) + jnp.einsum('bht,btc->bhc', rounded(suffix_exp), own_latent)
            latent_out = rounded(gathered / row_total[..., None])
            expanded = jnp.einsum('bhc,hcv->bhv', latent_out, value_weight)
            return expanded.astype(jnp.bfloat16).reshape(SEQ_DEV, HEADS * VDIM)

        items = (
            query_nope[layer_index].reshape(groups, SEQ_DEV, HEADS, NOPE),
            query_rope[layer_index].reshape(groups, SEQ_DEV, HEADS, ROPE),
            suffix_latent[layer_index].reshape(groups, SEQ_DEV, SUF, RANK),
            suffix_rope[layer_index].reshape(groups, SEQ_DEV, ROPE, SUF),
            lengths.reshape(groups, SEQ_DEV),
        )
        blocks_out = lax.map(one_block, items)
        results.append(blocks_out.reshape(SEQS, HEADS * VDIM))
    return jnp.stack(results)
```

```python
import jax
import jax.numpy as jnp
from jax import lax
from jax.sharding import PartitionSpec as P

HEADS = 16
NOPE = 128
ROPE = 64
VDIM = 128
AXES = ("dp", "head")
SIZE = {"x": 4, "y": 4, "z": 8, "core": 2}


def flat(x, y, z, core):
    z_hi, z_lo = divmod(z, 4)
    return (z_hi * 2 + core) * 64 + x * 16 + y * 4 + z_lo


def fetch(value, axis, offset):
    pairs = []
    for x in range(4):
        for y in range(4):
            for z in range(8):
                for core in range(2):
                    at = {"x": x, "y": y, "z": z, "core": core}
                    source = dict(at)
                    source[axis] = (at[axis] + offset) % SIZE[axis]
                    pairs.append((flat(**source), flat(**at)))
    return lax.ppermute(value, AXES, pairs)


def line(piece, axis, dim):
    parts = [piece] + [fetch(piece, axis, d) for d in (1, 2, -1)]
    return jnp.concatenate(parts, axis=dim)


def line_relayed(piece, axis):
    half = piece.shape[0] // 2
    right = fetch(piece, axis, 1)
    left = fetch(piece, axis, -1)
    opposite_low = fetch(right[:half], axis, 1)
    opposite_high = fetch(left[half:], axis, -1)
    return [piece, right, opposite_low, opposite_high, left]


def at_place(parts, first, dim):
    width = parts.shape[dim] // 4
    blocks = [
        lax.dynamic_slice_in_dim(parts, ((k - first) % 4) * width, width, axis=dim) for k in range(4)
    ]
    return blocks


def far_weights(weight, x, y):
    layers, heads, rows, lanes = weight.shape
    quarter = rows // 4
    piece = lax.dynamic_slice(weight, (0, x, y * quarter, 0), (layers, 1, quarter, lanes))
    piece = fetch(piece, "z", 4)
    lower, upper = piece[:1], piece[1:]
    lower = line(line(lower, "x", 1), "y", 2)
    upper = line(line(upper, "y", 2), "x", 1)
    both = jnp.concatenate([lower, upper], axis=0)
    both = jnp.concatenate(at_place(both, x, 1), axis=1)
    return jnp.concatenate(at_place(both, y, 2), axis=2)


def all_weights(weight, x, y):
    far = far_weights(weight, x, y)
    near = fetch(weight, "core", 1)
    far_near = fetch(far, "core", 1)
    return jnp.concatenate([weight, near, far, far_near], axis=1)


def by_xor(value, dp, dim):
    return jnp.concatenate(
        [lax.dynamic_slice_in_dim(value, dp ^ k, 1, axis=dim) for k in range(4)], axis=dim
    )


def gathered_pool(pool_latent, pool_rope, core):
    layers = pool_latent.shape[0]
    latent = lax.dynamic_slice_in_dim(pool_latent[:, 0], core * 64, 64, axis=1)
    rope = lax.dynamic_slice_in_dim(pool_rope[:, 0], core * 64, 64, axis=2)
    rope = rope.reshape(layers, ROPE, 8, 8).transpose(0, 3, 2, 1).reshape(layers, 8, 512)
    block = jnp.concatenate([latent, rope], axis=1)[:, None]
    orders = ("xyz", "yzx", "zxy")
    pieces = []
    for k, order in enumerate(orders):
        piece = block[:, :, 24 * k : 24 * k + 24]
        piece = line(piece, order[0], 1)
        piece = line(piece, order[1], 1)
        pieces.append(piece)
    results = []
    for layer in range(layers):
        thirds = []
        for order, piece in zip(orders, pieces):
            third = jnp.concatenate(line_relayed(piece[layer], order[2]), axis=0)
            third = third.reshape(4, 4, 4, 24, 512)
            names = order[::-1]
            third = third.transpose(*(names.index(a) for a in "xyz"), 3, 4)
            thirds.append(third.reshape(64, 24, 512))
        latents = jnp.concatenate([thirds[0], thirds[1], thirds[2][:, :16]], axis=1)
        ropes = thirds[2][:, 16:].reshape(64, 8, 8, ROPE).transpose(0, 2, 1, 3)
        results.append((latents.reshape(4096, 512), ropes.reshape(4096, ROPE)))
    return results


def on_device(
    query_nope,
    query_rope,
    key_up,
    value_up,
    pool_latent,
    pool_rope,
    block_table,
    suffix_latent,
    suffix_rope,
    lengths,
):
    layers, sequences = query_nope.shape[:2]
    rows = sequences * HEADS
    scale = (NOPE + ROPE) ** (-0.5)
    dp = lax.axis_index("dp")
    head = lax.axis_index("head")
    x, y, z = head // 16, (head // 4) % 4, head % 4
    core = dp % 2
    keys = all_weights(key_up, x, y)
    pool = gathered_pool(pool_latent, pool_rope, core)
    values = all_weights(value_up, x, y)
    offsets = jnp.arange(64, dtype=jnp.int32)
    slots = (
        ((x + offsets // 16) % 4) * 16 + ((y + (offsets // 4) % 4) % 4) * 4 + (z + offsets % 4) % 4
    )
    used = jnp.any(block_table[:, :, None] == slots[None, None, :], axis=1)
    results = []
    for layer in range(layers):
        q_nope = by_xor(query_nope[layer].reshape(sequences, 4, 4 * NOPE), dp, 1)
        q_rope = by_xor(query_rope[layer].reshape(sequences, 4, 4 * ROPE), dp, 1)
        q_nope = q_nope.reshape(sequences, HEADS, NOPE)
        q_rope = q_rope.reshape(sequences, HEADS, ROPE)
        q_latent = jnp.einsum(
            "shd,hdc->shc", q_nope, keys[layer], preferred_element_type=jnp.float32
        ).astype(jnp.bfloat16)
        both_latent = jnp.concatenate(
            [q_latent.reshape(rows, -1), fetch(q_latent.reshape(rows, -1), "core", 1)], axis=0
        )
        both_rope = jnp.concatenate(
            [q_rope.reshape(rows, -1), fetch(q_rope.reshape(rows, -1), "core", 1)], axis=0
        )
        own_latent = suffix_latent[layer]
        own_scores = jnp.einsum(
            "shc,stc->sht", q_latent, own_latent, preferred_element_type=jnp.float32
        )
        own_scores = own_scores + jnp.einsum(
            "shr,srt->sht", q_rope, suffix_rope[layer], preferred_element_type=jnp.float32
        )
        own_scores = own_scores * scale
        live = (jnp.arange(own_latent.shape[1])[None, :] < lengths[:, None])[:, None, :]
        own_max = jnp.max(jnp.where(live, own_scores, -jnp.inf), axis=2)
        own_weights = jnp.where(live, jnp.exp(own_scores - own_max[..., None]), 0.0)
        own_sum = jnp.sum(own_weights, axis=2).reshape(rows)
        own_out = jnp.einsum(
            "sht,stc->shc",
            own_weights.astype(jnp.bfloat16),
            own_latent,
            preferred_element_type=jnp.float32,
        ).reshape(rows, -1)
        own_max = own_max.reshape(rows)
        latents, ropes = pool[layer]
        scores = jnp.einsum("nc,tc->nt", both_latent, latents, preferred_element_type=jnp.float32)
        scores = scores + jnp.einsum(
            "nr,tr->nt", both_rope, ropes, preferred_element_type=jnp.float32
        )
        mask = jnp.repeat(used[layer], 64)[None, :]
        scores = jnp.where(mask, scores * scale, -jnp.inf)
        top = jnp.max(scores, axis=1)
        weights = jnp.exp(scores - top[:, None])
        sums = jnp.sum(weights, axis=1)
        part = jnp.einsum(
            "nt,tc->nc",
            weights.astype(jnp.bfloat16),
            latents,
            preferred_element_type=jnp.float32,
        )
        other_part = fetch(part[rows:], "core", 1)
        other = fetch(jnp.stack([top[rows:], sums[rows:]]), "core", 1)
        best = jnp.maximum(jnp.maximum(top[:rows], other[0]), own_max)
        f_here = jnp.exp(top[:rows] - best)
        f_other = jnp.exp(other[0] - best)
        f_own = jnp.exp(own_max - best)
        total = sums[:rows] * f_here + other[1] * f_other + own_sum * f_own
        merged = (
            part[:rows] * f_here[:, None] + other_part * f_other[:, None] + own_out * f_own[:, None]
        )
        latent_out = (merged / total[:, None]).astype(jnp.bfloat16)
        expanded = jnp.einsum(
            "shc,hcv->shv",
            latent_out.reshape(sequences, HEADS, -1),
            values[layer],
            preferred_element_type=jnp.float32,
        ).astype(jnp.bfloat16)
        expanded = by_xor(expanded.reshape(sequences, 4, 4 * VDIM), dp, 1)
        results.append(expanded.reshape(sequences, HEADS * VDIM))
    return jnp.stack(results)


def solution(mesh):
    return jax.shard_map(
        on_device,
        mesh=mesh,
        in_specs=(
            P(None, ("dp", "head"), None),
            P(None, ("dp", "head"), None),
            P(None, "dp", None, None),
            P(None, "dp", None, None),
            P(None, "head", None, None),
            P(None, "head", None, None),
            P(),
            P(None, ("dp", "head"), None, None),
            P(None, ("dp", "head"), None, None),
            P(("dp", "head")),
        ),
        out_specs=P(None, ("dp", "head"), None),
        check_vma=False,
    )
```

```python
import functools
import math

import jax
import jax.numpy as jnp
from jax import lax
from jax.experimental import pallas as pl
from jax.experimental.pallas import tpu as pltpu
from jax.sharding import PartitionSpec as P


HEADS = 16
RANK = 512
NOPE = 128
ROPE = 64
VDIM = 128
HALF = 64
PACK = 72
WIDE = 640
FAR_BELOW = -1e30
GROUP = 8
CHUNK = GROUP * HALF
AXES = ("dp", "head")
ORDER = (0, 2, 1, 3)
SIZE = {"x": 4, "y": 4, "z": 8, "core": 2}
SCALE = (NOPE + ROPE) ** (-0.5)
SCALE2 = SCALE * math.log2(math.e)


def flat(x, y, z, core):
    z_hi, z_lo = divmod(z, 4)
    return (z_hi * 2 + core) * 64 + x * 16 + y * 4 + z_lo


def fetch(value, axis, offset):
    pairs = []
    for x in range(4):
        for y in range(4):
            for z in range(8):
                for core in range(2):
                    at = {"x": x, "y": y, "z": z, "core": core}
                    source = dict(at)
                    source[axis] = (at[axis] + offset) % SIZE[axis]
                    pairs.append((flat(**source), flat(**at)))
    return lax.ppermute(value, AXES, pairs)


def attend_kernel(n_pieces, n_states, used, q, *refs):
    pieces = refs[:n_pieces]
    states = refs[n_pieces : n_pieces + n_states]
    refs = refs[n_pieces + n_states :]
    out = refs[:2]
    keys, scores, gathered, tops, sums = refs[2:]
    rows = q.shape[0]
    half = rows // 2

    count = jnp.int32(0)
    for k, piece in enumerate(pieces):
        per = piece.shape[0]

        def pack(i, count, piece=piece, base=k * per):
            at = pl.multiple_of(count * HALF, HALF)
            keys[pl.ds(at, HALF), :RANK] = piece[i, :HALF, :]
            for j in range(4):
                pair = piece[i, HALF:, 2 * ROPE * j : 2 * ROPE * (j + 1)]
                rope = jnp.concatenate([pair[:, :ROPE], pair[:, ROPE:]], axis=0)
                rope = jnp.concatenate([rope, jnp.zeros_like(rope)], axis=1)
                keys[pl.ds(at + 16 * j, 16), RANK:] = rope
            return count + used[base + i]

        count = lax.fori_loop(0, per, pack, count)
    tail = pl.multiple_of(count * HALF, HALF)
    keys[pl.ds(tail, CHUNK), :RANK] = jnp.zeros((CHUNK, RANK), jnp.bfloat16)
    lane = lax.broadcasted_iota(jnp.int32, (CHUNK, WIDE - RANK), 1)
    below = jnp.where(lane == ROPE, FAR_BELOW, 0.0).astype(jnp.bfloat16)
    keys[pl.ds(tail, CHUNK), RANK:] = below
    whole = (count + GROUP // 2 - 1) // GROUP
    rest = (count + GROUP - 1) // GROUP - whole

    for r in range(2):
        at = slice(half * r, half * (r + 1))
        if r < n_states:
            tops[at] = jnp.broadcast_to(states[r][:, RANK : RANK + 1], (half, 128))
        else:
            tops[at] = jnp.full((half, 128), FAR_BELOW, jnp.float32)

    def score(c, size):
        at = pl.multiple_of(c * CHUNK, CHUNK)
        s = lax.dot_general(
            q[...],
            keys[pl.ds(at, size), :],
            (((1,), (1,)), ((), ())),
            preferred_element_type=jnp.float32,
        )
        scores[c, :, :size] = s
        best = tops[...]
        for k in range(size // 128):
            best = jnp.maximum(best, s[:, 128 * k : 128 * (k + 1)])
        tops[...] = best

    @pl.loop(0, whole)
    def _(c):
        score(c, CHUNK)

    @pl.when(rest > 0)
    def _():
        score(whole, CHUNK // 2)

    top = jnp.broadcast_to(jnp.max(tops[...], axis=1, keepdims=True), (rows, 128))
    tops[...] = top
    first = lax.broadcasted_iota(jnp.int32, (half, 128), 1) == 0
    for r in range(2):
        at = slice(half * r, half * (r + 1))
        if r < n_states:
            old = states[r][:, RANK : RANK + 1]
            factor = jnp.exp2((old - top[at][:, :1]) * SCALE2)
            gathered[at] = states[r][:, :RANK] * factor
            sums[at] = jnp.where(first, states[r][:, RANK + 64 : RANK + 65] * factor, 0.0)
        else:
            gathered[at] = jnp.zeros((half, RANK), jnp.float32)
            sums[at] = jnp.zeros((half, 128), jnp.float32)

    def fold(c, size):
        at = pl.multiple_of(c * CHUNK, CHUNK)
        top = tops[...]
        parts = [
            jnp.exp2((scores[c, :, 128 * k : 128 * (k + 1)] - top) * SCALE2)
            for k in range(size // 128)
        ]
        sums[...] += sum(parts[1:], parts[0])
        weights = jnp.concatenate([p.astype(jnp.bfloat16) for p in parts], axis=1)
        gathered[...] += jnp.dot(
            weights, keys[pl.ds(at, size), :RANK], preferred_element_type=jnp.float32
        )

    @pl.loop(0, whole)
    def _(c):
        fold(c, CHUNK)

    @pl.when(rest > 0)
    def _():
        fold(whole, CHUNK // 2)

    lane = lax.broadcasted_iota(jnp.int32, (half, 128), 1)
    total = jnp.sum(sums[...], axis=1, keepdims=True)
    for r in range(2):
        at = slice(half * r, half * (r + 1))
        out[r][:, :RANK] = gathered[at]
        out[r][:, RANK:] = jnp.where(lane < 64, tops[at], total[at])


def attend(used, q, pieces, states):
    slots = sum(p.shape[0] for p in pieces)
    operands = [used, q, *pieces, *states]
    rows = q.shape[0]
    tokens = slots * 48
    vmem = pl.BlockSpec(memory_space=pltpu.VMEM)
    return pl.pallas_call(
        functools.partial(attend_kernel, len(pieces), len(states)),
        out_shape=[jax.ShapeDtypeStruct((rows // 2, WIDE), jnp.float32)] * 2,
        in_specs=[pl.BlockSpec(memory_space=pltpu.SMEM)] + [vmem] * (len(operands) - 1),
        out_specs=[vmem] * 2,
        scratch_shapes=[
            pltpu.VMEM(((slots + GROUP) * HALF, WIDE), jnp.bfloat16),
            pltpu.VMEM((slots // GROUP, rows, CHUNK), jnp.float32),
            pltpu.VMEM((rows, RANK), jnp.float32),
            pltpu.VMEM((rows, 128), jnp.float32),
            pltpu.VMEM((rows, 128), jnp.float32),
        ],
        compiler_params=pltpu.CompilerParams(vmem_limit_bytes=20 * 1024 * 1024),
        cost_estimate=pl.CostEstimate(
            flops=2 * rows * tokens * (WIDE + RANK),
            bytes_accessed=slots * PACK * RANK * 2,
            transcendentals=rows * tokens,
        ),
    )(*operands)


def finish_kernel(heads, here, other, *refs):
    values = refs[:4]
    out = refs[-1]
    states = (here, other)
    tops = [s[:, RANK : RANK + 1] for s in states]
    best = jnp.maximum(tops[0], tops[1])
    factors = [jnp.exp2((t - best) * SCALE2) for t in tops]
    total = sum(s[:, RANK + 64 : RANK + 65] * f for s, f in zip(states, factors))
    merged = sum(s[:, :RANK] * f for s, f in zip(states, factors))
    latent_out = (merged / total).astype(jnp.bfloat16)
    for k in range(0, HEADS, 2):
        pair = [values[j // 4][j % 4] for j in (k, k + 1)]
        both = jnp.dot(
            latent_out[16 * k : 16 * (k + 2)],
            jnp.concatenate(pair, axis=1),
            preferred_element_type=jnp.float32,
        ).astype(jnp.bfloat16)
        for j in range(2):
            at = pl.multiple_of(heads[k + j] * VDIM, VDIM)
            out[:, pl.ds(at, VDIM)] = both[16 * j : 16 * (j + 1), VDIM * j : VDIM * (j + 1)]


def finish(layer, heads, here, other, values, result):
    state = pl.BlockSpec((256, WIDE), lambda i: (0, 0))
    value = pl.BlockSpec((None, 4, RANK, VDIM), lambda i: (layer, 0, 0, 0))
    operands = [heads, here, other, *values]
    specs = [pl.BlockSpec(memory_space=pltpu.SMEM), state, state] + [value] * 4
    aliases = {}
    if result is not None:
        operands.append(result)
        specs.append(pl.BlockSpec(memory_space=pl.ANY))
        aliases = {len(operands) - 1: 0}
    return pl.pallas_call(
        finish_kernel,
        grid=(1,),
        out_shape=jax.ShapeDtypeStruct((2, 16, HEADS * VDIM), jnp.bfloat16),
        in_specs=specs,
        out_specs=pl.BlockSpec((None, 16, HEADS * VDIM), lambda i: (layer, 0, 0)),
        input_output_aliases=aliases,
        compiler_params=pltpu.CompilerParams(vmem_limit_bytes=12 * 1024 * 1024),
        cost_estimate=pl.CostEstimate(
            flops=2 * 256 * RANK * VDIM, bytes_accessed=4 * 1024 * 1024, transcendentals=1024
        ),
    )(*operands)


def small_call(kernel, shapes, operands, scalars=0):
    vmem = pl.BlockSpec(memory_space=pltpu.VMEM)
    smem = pl.BlockSpec(memory_space=pltpu.SMEM)
    size = sum(math.prod(shape) * 2 for shape in shapes)
    return pl.pallas_call(
        kernel,
        out_shape=[jax.ShapeDtypeStruct(shape, jnp.bfloat16) for shape in shapes],
        in_specs=[smem] * scalars + [vmem] * (len(operands) - scalars),
        out_specs=[vmem] * len(shapes),
        compiler_params=pltpu.CompilerParams(vmem_limit_bytes=8 * 1024 * 1024),
        cost_estimate=pl.CostEstimate(flops=size, bytes_accessed=2 * size, transcendentals=0),
    )(*operands)


def split_kernel(dp, nope, rope, mine, far, sent, ropes):
    wide, narrow = 4 * NOPE, 4 * ROPE
    for out, k in ((mine, 0), (far, 2)):
        out[...] = nope[:, :, pl.ds(pl.multiple_of((dp[0] ^ k) * wide, wide), wide)]
    for place, k in enumerate((1, 3)):
        block = nope[:, :, pl.ds(pl.multiple_of((dp[0] ^ k) * wide, wide), wide)]
        sent[:, :, place * wide : (place + 1) * wide] = block
    for place, k in enumerate(ORDER):
        block = rope[:, :, pl.ds(pl.multiple_of((dp[0] ^ k) * narrow, narrow), narrow)]
        ropes[:, :, place * narrow : (place + 1) * narrow] = block
        at = 2 * wide + place * narrow
        sent[:, :, at : at + narrow] = block


def pair_kernel(mine, far, theirs, local, guest, ropes):
    wide, n = 4 * NOPE, mine.shape[1]
    local[:, :n] = mine[...]
    local[:, n:] = theirs[:, :, :wide]
    guest[:, :n] = far[...]
    guest[:, n:] = theirs[:, :, wide : 2 * wide]
    ropes[...] = theirs[:, :, 2 * wide :]


def compose_kernel(eight, other_eight, rope_here, rope_there, q, latent):
    n = latent.shape[2]
    lane = lax.broadcasted_iota(jnp.int32, (n, WIDE - RANK - ROPE), 1)
    one = jnp.where(lane == 0, 1.0, 0.0).astype(jnp.bfloat16)
    for layer in range(2):
        for h in range(HEADS):
            mine = eight if h < 8 else other_eight
            seen = mine[layer, h % 8, :n] if h < 8 else mine[layer, h % 8, n:]
            latent[layer, h] = seen
            theirs = other_eight if h < 8 else eight
            at = n * h
            q[layer, at : at + n, :RANK] = seen
            rope = rope_here[layer, :, ROPE * h : ROPE * (h + 1)]
            q[layer, at : at + n, RANK:] = jnp.concatenate([rope, one], axis=1)
            at = n * (HEADS + h)
            seen = theirs[layer, h % 8, :n] if h < 8 else theirs[layer, h % 8, n:]
            q[layer, at : at + n, :RANK] = seen
            rope = rope_there[layer, :, ROPE * h : ROPE * (h + 1)]
            q[layer, at : at + n, RANK:] = jnp.concatenate([rope, one], axis=1)


def rows_kernel(*refs):
    for k in range(4):
        for layer in range(2):
            refs[4 + layer][k] = refs[k][layer, 0]


def plane_kernel(*refs):
    for k in range(4):
        refs[4][4 * k : 4 * (k + 1)] = refs[k][...]


def own_blocks(pool_latent, pool_rope, core):
    layers = pool_latent.shape[0]
    latent = lax.dynamic_slice_in_dim(pool_latent[:, 0], core * HALF, HALF, axis=1)
    rope = lax.dynamic_slice_in_dim(pool_rope[:, 0], core * HALF, HALF, axis=2)
    rope = rope.reshape(layers, ROPE, 8, 8).transpose(0, 3, 2, 1).reshape(layers, 8, RANK)
    return jnp.concatenate([latent, rope], axis=1)[:, None]


def on_device(
    query_nope,
    query_rope,
    key_up,
    value_up,
    pool_latent,
    pool_rope,
    block_table,
    suffix_latent,
    suffix_rope,
    lengths,
):
    layers, sequences = query_nope.shape[:2]
    rows = sequences * HEADS
    dp = lax.axis_index("dp")
    head = lax.axis_index("head")
    place = {"x": head // 16, "y": (head // 4) % 4, "z": head % 4}
    core = dp % 2
    n, wide = sequences, 4 * NOPE
    own_dp = dp.astype(jnp.int32).reshape(1)
    mine, far, sent, rope_flat = small_call(
        split_kernel,
        [(layers, n, wide), (layers, n, wide), (layers, n, 4 * wide), (layers, n, 2 * wide)],
        [own_dp, query_nope, query_rope],
        scalars=1,
    )
    theirs = fetch(sent, "core", 1)
    block = own_blocks(pool_latent, pool_rope, core)
    by_z = [block] + [fetch(block, "z", d) for d in (1, 2, -1)]
    local, guest, rope_theirs = small_call(
        pair_kernel,
        [(layers, 2 * n, wide), (layers, 2 * n, wide), (layers, n, 2 * wide)],
        [mine, far, theirs],
    )
    guests = fetch(guest, "z", 4)
    held = jnp.concatenate([local, guests], axis=1).reshape(layers, 4 * sequences, 4, NOPE)
    absorbed = jnp.einsum(
        "lshd,lhdc->lhsc", held, key_up, preferred_element_type=jnp.float32
    ).astype(jnp.bfloat16)
    returned = fetch(absorbed[:, :, 2 * sequences :], "z", 4)
    eight = jnp.concatenate([absorbed[:, :, : 2 * sequences], returned], axis=1)
    other_eight = fetch(eight, "core", 1)

    orders = ("zyx", "zxy")
    row_shape, plane_shape = (4, PACK, RANK), (16, PACK, RANK)
    pool_rows = small_call(rows_kernel, [row_shape] * 2, by_z)
    parts = []
    for row, order in zip(pool_rows, orders):
        parts.append([row] + [fetch(row, order[1], d) for d in (1, 2, -1)])
    planes = [small_call(plane_kernel, [plane_shape], part)[0] for part in parts]
    far_value = fetch(value_up, "z", 4)
    near_value = fetch(value_up, "core", 1)
    last_value = fetch(far_value, "core", 1)
    values = (value_up, far_value, near_value, last_value)
    sides = []
    for plane, order in zip(planes, orders):
        sides.append((fetch(plane, order[2], 1), fetch(plane, order[2], -1)))
    opposites = []
    for (right, left), order in zip(sides, orders):
        opposites.append((fetch(right[:8], order[2], 1), fetch(left[8:], order[2], -1)))

    used = []
    for layer, order in enumerate(orders):
        turn = jnp.array([0, 1, 3, 2], jnp.int32)
        at = {
            order[0]: (place[order[0]] + jnp.arange(4, dtype=jnp.int32)[None, None, :]) % 4,
            order[1]: (place[order[1]] + jnp.arange(4, dtype=jnp.int32)[None, :, None]) % 4,
            order[2]: (place[order[2]] + turn[:, None, None]) % 4,
        }
        slot = (at["x"] * 16 + at["y"] * 4 + at["z"]).reshape(64)
        found = jnp.any(block_table[layer][:, None] == slot[None, :], axis=0)
        used.append(found.astype(jnp.int32))

    def by_head(ropes):
        ropes = ropes.reshape(layers, sequences, HEADS, ROPE).transpose(0, 2, 1, 3)
        return ropes.reshape(layers, rows, ROPE)

    q_both, latent_here = small_call(
        compose_kernel,
        [(layers, 2 * rows, WIDE), (layers, HEADS, n, RANK)],
        [eight, other_eight, rope_flat, rope_theirs],
    )
    rope_here = by_head(rope_flat)

    q_rope = rope_here.reshape(layers, HEADS, sequences, ROPE)
    live = (jnp.arange(suffix_latent.shape[2])[None, :] < lengths[:, None])[None, :, None, :]
    own_scores = jnp.einsum(
        "lhsc,lstc->lsht", latent_here, suffix_latent, preferred_element_type=jnp.float32
    )
    own_scores = own_scores + jnp.einsum(
        "lhsr,lsrt->lsht", q_rope, suffix_rope, preferred_element_type=jnp.float32
    )
    own_top = jnp.max(jnp.where(live, own_scores, -jnp.inf), axis=3, keepdims=True)
    own_weights = jnp.where(live, jnp.exp2((own_scores - own_top) * SCALE2), 0.0)
    own_sum = jnp.sum(own_weights, axis=3, keepdims=True)
    own_out = jnp.einsum(
        "lsht,lstc->lshc",
        own_weights.astype(jnp.bfloat16),
        suffix_latent,
        preferred_element_type=jnp.float32,
    )
    pad = (layers, sequences, HEADS, 64)
    own = jnp.concatenate(
        [own_out, jnp.broadcast_to(own_top, pad), jnp.broadcast_to(own_sum, pad)], axis=3
    )
    own = own.transpose(0, 2, 1, 3).reshape(layers, rows, WIDE)

    places = jnp.concatenate(
        [(dp ^ k) * 4 + jnp.arange(4, dtype=jnp.int32) for k in ORDER]
    ).astype(jnp.int32)
    states = []
    for layer in range(layers):
        states.append(attend(used[layer][:16], q_both[layer], (planes[layer],), (own[layer],)))
    states = [attend(used[k][16:48], q_both[k], sides[k], states[k]) for k in range(layers)]
    result = None
    merged = []
    for layer in range(layers):
        here, there = attend(used[layer][48:], q_both[layer], opposites[layer], states[layer])
        merged.append((here, fetch(there, "core", 1)))
    for layer, (here, other) in enumerate(merged):
        result = finish(layer, places, here, other, values, result)
    return result


def solution(mesh):
    return jax.shard_map(
        on_device,
        mesh=mesh,
        in_specs=(
            P(None, ("dp", "head"), None),
            P(None, ("dp", "head"), None),
            P(None, "dp", None, None),
            P(None, "dp", None, None),
            P(None, "head", None, None),
            P(None, "head", None, None),
            P(),
            P(None, ("dp", "head"), None, None),
            P(None, ("dp", "head"), None, None),
            P(("dp", "head")),
        ),
        out_specs=P(None, ("dp", "head"), None),
        check_vma=False,
    )
```
